32 devices in a mesh: member: 2 (over y), wave: 4 (over x, core), lev: 4 (over z).
Axes of the slice: x: 2, y: 2, z: 4, core: 2. Of those that a mesh axis runs over, the one named last changes fastest.
Arguments:
- grid_fields: bfloat16 [4, 64, 512, 1024], P('member', 'lev', 'wave'), parts along dimension 0, may hold values from -6 to 6
- band_latitude: int32 [512], replicated, may hold values from 0 to 511, as said below
- wave_of_slot: int32 [512], replicated, may hold values from 0 to 511, as said below
- legendre: bfloat16 [512, 2, 256, 256], P('wave'), may hold values from -0.25 to 0.25
- quad_weight: float32 [256], replicated, may hold values from 0.5 to 1.5
- wave_speed: float32 [128], P('member'), parts along dimension 0, may hold values from 0.5 to 4
- layer_depth: float32 [128], P('member'), parts along dimension 0, may hold values from 0.25 to 2
- diffusion: float32 [128], P('member'), parts along dimension 0, may hold values from 0.5 to 8
Outputs:
- grid_out: bfloat16 [4, 64, 512, 1024], P('member', 'lev', 'wave'), parts along dimension 0
The draws below stay inside these ranges and needn't reach their ends.
There are 2 independent parts, one for each index of `member`. The reference program is written for one: setup_inputs(seed, part) draws one part's arguments, and reference() takes and returns one part's arrays. A program takes and returns all parts, laid end to end along the dimension named above; an argument that names none is the same for every part. Nothing has to cross between parts.
Inputs may be any that keep to these rules, and one draw needn't show every extreme that they name: `wave_of_slot`: A permutation of the 512 wavenumbers in which slots 2 k and 2 k + 1 hold a wavenumber m < 256 and 511 - m. `band_latitude`: A permutation of the 512 latitudes; each aligned block of 128 rows holds 64 latitudes i < 256 followed by their mirrors 512 - 1 - i in the same order.
All inputs are finite; a program needn't handle non-finite values.
Results may differ from the reference program's by a relative error of at most 0.017.
Values may be sent and summed in bfloat16 or wider, within the bound.
A program may use at most 192 MiB of HBM per device.

```python
import math
import jax
import jax.numpy as jnp
from jax import lax

NLON = 1024
NLAT = 512
MW = 512
FIELDS = 2
LEVELS = 64
LAT_DEV = 128


def draw_wave_of_slot(key, part):
    lower = jax.random.permutation(jax.random.fold_in(key, 11), MW // 2).astype(jnp.int32)
    return jnp.stack([lower, MW - 1 - lower], axis=1).reshape(MW)


def draw_band_latitude(key, part):
    northern = jax.random.permutation(jax.random.fold_in(key, 12), NLAT // 2).astype(jnp.int32)
    northern = northern.reshape(NLAT // LAT_DEV, LAT_DEV // 2)
    return jnp.concatenate([northern, NLAT - 1 - northern], axis=1).reshape(NLAT)


def levels(rng, dims, cuts, least, largest):
    loudness, own = 1.0, jax.random.fold_in(rng, 6)
    for axis_at, parts in cuts:
        draws = jnp.exp(jax.random.uniform(jax.random.fold_in(own, axis_at), (parts,), jnp.float32, least / len(cuts), largest / len(cuts)))
        loudness = loudness * jnp.repeat(draws, dims[axis_at] // parts).reshape([-1 if axis == axis_at else 1 for axis in range(len(dims))])
    return loudness


def bell_draw(own_key, dims, spread, reach, shards=(), kind=jnp.bfloat16):
    drawn = jax.random.normal(own_key, dims, jnp.float32) * spread
    if len(shards) > 0:
        drawn = levels(own_key, dims, shards, -0.22, 0.18) * drawn
    return jnp.clip(drawn, min=-reach, max=reach).astype(kind)


def setup_inputs(seed: int = 0, part: int = 0) -> dict:
    key_list = jax.random.split(jax.random.key(seed), 9)
    own_keys = jax.random.split(jax.random.fold_in(key_list[8], part), 9)
    return {
        "grid_fields": bell_draw(own_keys[0], (FIELDS, LEVELS, NLAT, NLON), 1.0, 6.0, ((1, 4), (2, 4))),
        "band_latitude": draw_band_latitude(jax.random.fold_in(key_list[8], 71), part),
        "wave_of_slot": draw_wave_of_slot(jax.random.fold_in(key_list[8], 71), part),
        "legendre": bell_draw(key_list[3], (MW, 2, NLAT // 2, MW // 2), NLAT ** -0.5, 0.25, ((0, 4),)),
        "quad_weight": jnp.clip(jax.random.uniform(key_list[4], (NLAT // 2,), jnp.float32, 0.5, 1.5), 0.5, 1.5),
        "wave_speed": jnp.clip(jnp.exp(jax.random.uniform(own_keys[5], (LEVELS,), jnp.float32, math.log(0.5), math.log(4.0))), 0.5, 4.0),
        "layer_depth": jnp.clip(jnp.exp(jax.random.uniform(own_keys[6], (LEVELS,), jnp.float32, math.log(0.25), math.log(2.0))), 0.25, 2.0),
        "diffusion": jnp.clip(jnp.exp(jax.random.uniform(own_keys[7], (LEVELS,), jnp.float32, math.log(0.5), math.log(8.0))), 0.5, 8.0),
    }


def dynamics(spectrum, degree, wave_speed, layer_depth, diffusion):
    eigen_value = (degree * (degree + 1)).astype(jnp.float32) / float(MW * (MW - 1))
    eigen_value = eigen_value[None, :, None, :]
    speed_col = wave_speed[:, None, None, None]
    depth_col = layer_depth[:, None, None, None]
    diffusion_col = diffusion[:, None, None, None]
    divergence = spectrum[0]
    geopotential = spectrum[1]
    new_div = (divergence + speed_col * eigen_value * geopotential) / (1.0 + speed_col * depth_col * eigen_value)
    new_geo = geopotential - depth_col * new_div
    damping = jnp.where(degree[None, :, None, :] < MW, 1.0 / (1.0 + diffusion_col * eigen_value * eigen_value), 0.0)
    return jnp.stack([new_div * damping, new_geo * damping]).astype(jnp.bfloat16)

def reference(grid_fields, band_latitude, wave_of_slot, legendre, quad_weight, wave_speed, layer_depth, diffusion):
    north_count = NLAT // 2
    scaling = math.sqrt(2.0 / NLON)
    positions = jnp.arange(NLAT, dtype=jnp.int32)
    row_of_lat = jnp.zeros((NLAT,), jnp.int32).at[band_latitude].set(positions)
    north_rows = row_of_lat[:north_count]
    south_rows = row_of_lat[NLAT - 1 - jnp.arange(north_count, dtype=jnp.int32)]
    coeff_list = []
    for field_index in range(FIELDS):
        spectrum = jnp.fft.rfft(grid_fields[field_index].astype(jnp.float32), axis=-1)[..., wave_of_slot]
        parts_pair = jnp.stack([jnp.real(spectrum), jnp.imag(spectrum)], axis=-1) * scaling
        coeff_list.append(parts_pair.astype(jnp.bfloat16))
    fourier = jnp.stack(coeff_list)
    northern = fourier[:, :, north_rows].astype(jnp.float32)
    southern = fourier[:, :, south_rows].astype(jnp.float32)
    weights = quad_weight[:, None, None]
    symmetric = ((northern + southern) * weights).astype(jnp.bfloat16)
    antisymmetric = ((northern - southern) * weights).astype(jnp.bfloat16)
    legendre_full = legendre.astype(jnp.float32)
    columns = jnp.arange(MW // 2, dtype=jnp.int32)
    inverse_parts = []
    for parity, source in ((0, symmetric), (1, antisymmetric)):
        table_part = legendre_full[:, parity]
        spectral = jnp.einsum('flhsc,shj->flscj', source.astype(jnp.float32), table_part, precision=lax.Precision.HIGHEST)
        degree = wave_of_slot[:, None] + 2 * columns[None, :] + parity
        stepped = dynamics(spectral, degree, wave_speed, layer_depth, diffusion)
        inverse_parts.append(jnp.einsum('flscj,shj->flhsc', stepped.astype(jnp.float32), table_part, precision=lax.Precision.HIGHEST))
    even_part, odd_part = inverse_parts
    northern_out = (even_part + odd_part).astype(jnp.bfloat16)
    southern_out = (even_part - odd_part).astype(jnp.bfloat16)
    by_latitude = jnp.concatenate([northern_out, southern_out[:, :, ::-1]], axis=2)
    back = by_latitude[:, :, band_latitude].astype(jnp.float32)
    complex_part = back[..., 0] + 1j * back[..., 1]
    factors = jnp.where(wave_of_slot == 0, float(NLON), float(NLON // 2))
    full_spectrum = jnp.zeros(back.shape[:3] + (NLON // 2 + 1,), complex_part.dtype)
    full_spectrum = full_spectrum.at[..., wave_of_slot].set(complex_part * factors)
    grid = jnp.fft.irfft(full_spectrum, n=NLON, axis=-1) * scaling
    return grid.astype(jnp.bfloat16)
```

```python
import functools
import math

import jax
import jax.numpy as jnp
from jax import lax
from jax.experimental import pallas as pl
from jax.experimental.pallas import tpu as pltpu
from jax.sharding import PartitionSpec as P

CHUNKS = 4
VMEM_LIMIT = 60 * 1024 * 1024


def wave_table(wavenumbers, lon_count):
    longitudes = jnp.arange(lon_count, dtype=jnp.int32)
    phase = wavenumbers[..., None] * longitudes % lon_count
    angle = phase.astype(jnp.float32) * (2.0 * math.pi / lon_count)
    scaling = math.sqrt(2.0 / lon_count)
    stacked = jnp.stack([jnp.cos(angle) * scaling, -jnp.sin(angle) * scaling], axis=-3)
    return stacked.reshape(-1, lon_count).astype(jnp.bfloat16)


def dft_kernel(table_ref, grid_ref, *out_refs):
    block, rows, lon_count = grid_ref.shape
    piece_rows = out_refs[0].shape[1]
    result = lax.dot_general(
        table_ref[...],
        grid_ref[...].reshape(block * rows, lon_count),
        (((1,), (1,)), ((), ())),
        preferred_element_type=jnp.float32,
    ).astype(jnp.bfloat16)
    for part, out_ref in enumerate(out_refs):
        for item in range(block):
            out_ref[item] = result[
                part * piece_rows : (part + 1) * piece_rows, item * rows : (item + 1) * rows
            ]


def forward_dft(table, grid_rows, parts):
    items, rows, lon_count = grid_rows.shape
    table_rows = table.shape[0]
    piece_rows = table_rows // parts
    block = 4
    return pl.pallas_call(
        dft_kernel,
        grid=(items // block,),
        in_specs=[
            pl.BlockSpec((table_rows, lon_count), lambda i: (0, 0)),
            pl.BlockSpec((block, rows, lon_count), lambda i: (i, 0, 0)),
        ],
        out_specs=[pl.BlockSpec((block, piece_rows, rows), lambda i: (i, 0, 0))] * parts,
        out_shape=[jax.ShapeDtypeStruct((items, piece_rows, rows), jnp.bfloat16)] * parts,
        compiler_params=pltpu.CompilerParams(vmem_limit_bytes=VMEM_LIMIT),
        cost_estimate=pl.CostEstimate(
            flops=2 * table_rows * items * rows * lon_count,
            bytes_accessed=2 * (items * rows * lon_count + items * rows * table_rows),
            transcendentals=0,
        ),
        name="forward_dft",
    )(table, grid_rows)


def inverse_kernel(piece_count, *refs):
    piece_refs = refs[:piece_count]
    table_ref, out_ref = refs[piece_count], refs[piece_count + 1]
    block, rows, lon_count = out_ref.shape
    turned = []
    for item in range(block):
        column = jnp.concatenate([ref[item] for ref in piece_refs], axis=0)
        turned.append(column.T)
    left = jnp.concatenate(turned, axis=0)
    result = jnp.dot(left, table_ref[...], preferred_element_type=jnp.float32)
    out_ref[...] = result.astype(jnp.bfloat16).reshape(block, rows, lon_count)


def inverse_dft(pieces, table):
    items, piece_rows, rows = pieces[0].shape
    table_rows, lon_count = table.shape
    block = 4
    return pl.pallas_call(
        functools.partial(inverse_kernel, len(pieces)),
        grid=(items // block,),
        in_specs=[pl.BlockSpec((block, piece_rows, rows), lambda i: (i, 0, 0))] * len(pieces)
        + [pl.BlockSpec((table_rows, lon_count), lambda i: (0, 0))],
        out_specs=pl.BlockSpec((block, rows, lon_count), lambda i: (i, 0, 0)),
        out_shape=jax.ShapeDtypeStruct((items, rows, lon_count), jnp.bfloat16),
        compiler_params=pltpu.CompilerParams(vmem_limit_bytes=VMEM_LIMIT),
        cost_estimate=pl.CostEstimate(
            flops=2 * table_rows * items * rows * lon_count,
            bytes_accessed=2 * (items * rows * lon_count + items * rows * table_rows),
            transcendentals=0,
        ),
        name="inverse_dft",
    )(*pieces, table)


def legendre_kernel(piece_count, wave_count, waves_ref, *refs):
    piece_refs = refs[:piece_count]
    legendre_ref, fold_ref, unfold_ref, weight_ref, params_ref = refs[piece_count : piece_count + 5]
    out_refs = refs[piece_count + 5 : piece_count + 5 + piece_count]
    fold_scratch, back_scratch = refs[piece_count + 5 + piece_count :]
    items, comps, slots, rows = piece_refs[0].shape
    merged = items * comps
    half = merged // 2
    width = legendre_ref.shape[3]
    norths = legendre_ref.shape[2]
    lanes = fold_scratch.shape[2]
    tiles = fold_scratch.shape[0]
    per_parity = tiles // 2

    gathered = jnp.concatenate(
        [ref[...].reshape(merged * slots, rows) for ref in piece_refs], axis=1
    )
    for tile in range(tiles):
        columns = pl.ds(tile * lanes, lanes)
        fold_scratch[tile] = (
            jnp.dot(gathered, fold_ref[:, columns], preferred_element_type=jnp.float32)
            * weight_ref[:, columns]
        )

    first_slot = pl.program_id(0) * slots
    speed, depth, diffusion = params_ref[0], params_ref[1], params_ref[2]
    column_index = lax.broadcasted_iota(jnp.int32, (1, width), 1)

    def one_slot(slot, carry):
        wavenumber = waves_ref[first_slot + slot]
        picked = pl.ds(slot, merged, stride=slots)
        results = []
        for parity in range(2):
            source = jnp.concatenate(
                [
                    fold_scratch[parity * per_parity + tile, picked, :]
                    for tile in range(per_parity)
                ],
                axis=1,
            ).astype(jnp.bfloat16)
            table = legendre_ref[slot, parity]
            spectral = jnp.dot(source, table, preferred_element_type=jnp.float32)
            degree = wavenumber + 2 * column_index + parity
            eigen = (degree * (degree + 1)).astype(jnp.float32) * (
                1.0 / float(wave_count * (wave_count - 1))
            )
            divergence, geopotential = spectral[:half], spectral[half:]
            speed_eigen = speed * eigen
            new_div = (divergence + speed_eigen * geopotential) / (1.0 + speed_eigen * depth)
            new_geo = geopotential - depth * new_div
            damping = jnp.where(
                degree < wave_count, 1.0 / (1.0 + diffusion * (eigen * eigen)), 0.0
            )
            stepped = jnp.concatenate([new_div * damping, new_geo * damping], axis=0)
            results.append(
                lax.dot_general(
                    stepped.astype(jnp.bfloat16),
                    table,
                    (((1,), (1,)), ((), ())),
                    preferred_element_type=jnp.float32,
                )
            )
        north = results[0] + results[1]
        south = results[0] - results[1]
        for tile in range(per_parity):
            part = slice(tile * lanes, (tile + 1) * lanes)
            back_scratch[tile, picked, :] = north[:, part]
            back_scratch[per_parity + tile, picked, :] = south[:, part]
        return carry

    lax.fori_loop(0, slots, one_slot, 0, unroll=4)

    both = jnp.concatenate(
        [back_scratch[tile].astype(jnp.bfloat16) for tile in range(tiles)], axis=1
    )
    for part, out_ref in enumerate(out_refs):
        columns = pl.ds(part * rows, rows)
        out_ref[...] = (
            jnp.dot(both, unfold_ref[:, columns], preferred_element_type=jnp.float32)
            .astype(jnp.bfloat16)
            .reshape(items, comps, slots, rows)
        )


def legendre_step(pieces, waves, legendre, chunk, fold, unfold, weights, params, wave_count):
    items, comps, slots, rows = pieces[0].shape
    _, parities, norths, width = legendre.shape
    block = 16 if slots % 16 == 0 else slots
    steps = slots // block
    merged = items * comps
    all_rows = fold.shape[0]
    lanes = min(128, norths)
    tiles = 2 * norths // lanes
    piece_spec = pl.BlockSpec((items, comps, block, rows), lambda i, w: (0, 0, i, 0))

    def whole(array):
        return pl.BlockSpec(array.shape, lambda i, w: (0,) * array.ndim)

    return pl.pallas_call(
        functools.partial(legendre_kernel, len(pieces), wave_count),
        grid_spec=pltpu.PrefetchScalarGridSpec(
            num_scalar_prefetch=1,
            grid=(steps,),
            in_specs=[piece_spec] * len(pieces)
            + [
                pl.BlockSpec(
                    (block, parities, norths, width), lambda i, w: (chunk * steps + i, 0, 0, 0)
                ),
                whole(fold),
                whole(unfold),
                whole(weights),
                whole(params),
            ],
            out_specs=[piece_spec] * len(pieces),
            scratch_shapes=[
                pltpu.VMEM((tiles, merged * block, lanes), jnp.float32),
                pltpu.VMEM((tiles, merged * block, lanes), jnp.float32),
            ],
        ),
        out_shape=[jax.ShapeDtypeStruct(pieces[0].shape, jnp.bfloat16)] * len(pieces),
        compiler_params=pltpu.CompilerParams(vmem_limit_bytes=VMEM_LIMIT),
        cost_estimate=pl.CostEstimate(
            flops=2 * slots * merged * (4 * norths * width + 2 * all_rows * all_rows),
            bytes_accessed=2
            * (slots * parities * norths * width + 2 * slots * merged * all_rows),
            transcendentals=0,
        ),
        name="legendre_step",
    )(waves, *pieces, legendre, fold, unfold, weights, params)


def per_device(
    size,
    grid_fields,
    band_latitude,
    wave_of_slot,
    legendre,
    quad_weight,
    wave_speed,
    layer_depth,
    diffusion,
):
    field_count, lev_dev, lat_dev, lon_count = grid_fields.shape
    wave_count = wave_of_slot.shape[0]
    north_count = quad_weight.shape[0]
    half_band = lat_dev // 2
    slot_count = legendre.shape[0]
    width = legendre.shape[3]
    chunk_slots = slot_count // CHUNKS
    items = field_count * lev_dev
    me = lax.axis_index("wave")
    partners = jnp.bitwise_xor(me, jnp.arange(size, dtype=jnp.int32))

    level_start = lax.axis_index("lev") * lev_dev
    params = jnp.stack(
        [
            jnp.broadcast_to(
                jnp.repeat(lax.dynamic_slice_in_dim(values, level_start, lev_dev, 0), 2)[:, None],
                (2 * lev_dev, width),
            )
            for values in (wave_speed, layer_depth, diffusion)
        ]
    )

    waves = wave_of_slot.reshape(size, CHUNKS, chunk_slots)[partners]
    tables = [wave_table(waves[:, chunk], lon_count) for chunk in range(CHUNKS)]
    my_waves = waves[0]

    row_lat = band_latitude.reshape(size, lat_dev)[partners].reshape(size * lat_dev)
    lats = jnp.arange(north_count, dtype=jnp.int32)
    is_north = (row_lat[:, None] == lats[None, :]).astype(jnp.bfloat16)
    is_south = (row_lat[:, None] == 2 * north_count - 1 - lats[None, :]).astype(jnp.bfloat16)
    fold = jnp.concatenate([is_north + is_south, is_north - is_south], axis=1)
    unfold = jnp.concatenate([is_north, is_south], axis=1).T
    weights = jnp.concatenate([quad_weight, quad_weight])[None, :]

    def send(piece, offset):
        if offset == 0:
            return piece
        return lax.ppermute(piece, "wave", [(index, index ^ offset) for index in range(size)])

    grid_rows = grid_fields.reshape(items, lat_dev, lon_count)
    shape4 = (items, 2, chunk_slots, lat_dev)
    aligned = lat_dev % 128 == 0
    arrived = []
    for chunk in range(CHUNKS):
        pieces = forward_dft(tables[chunk], grid_rows, size)
        arrived.append([send(piece, offset) for offset, piece in enumerate(pieces)])
    returned = []
    for chunk in range(CHUNKS):
        pieces = [piece.reshape(shape4) for piece in arrived[chunk]]
        if not aligned:
            pieces = [jnp.concatenate(pieces, axis=3)]
        backs = legendre_step(
            pieces, my_waves[chunk], legendre, chunk, fold, unfold, weights, params, wave_count
        )
        if not aligned:
            backs = jnp.split(backs[0], size, axis=3)
        backs = [back.reshape(items, 2 * chunk_slots, lat_dev) for back in backs]
        returned += [send(back, offset) for offset, back in enumerate(backs)]
    table = jnp.concatenate(tables, axis=0)
    grid_out = inverse_dft(returned, table)
    return grid_out.reshape(field_count, lev_dev, lat_dev, lon_count)


def solution(mesh):
    in_specs = (
        P("member", "lev", "wave", None),
        P(),
        P(),
        P("wave", None, None, None),
        P(),
        P("member"),
        P("member"),
        P("member"),
    )
    out_specs = P("member", "lev", "wave", None)
    return jax.shard_map(
        functools.partial(per_device, mesh.shape["wave"]),
        mesh=mesh,
        in_specs=in_specs,
        out_specs=out_specs,
        check_vma=False,
    )
```

```python
import functools
import math

import jax
import jax.numpy as jnp
from jax import lax
from jax.experimental import pallas as pl
from jax.experimental.pallas import tpu as pltpu
from jax.sharding import PartitionSpec as P

CHUNKS = 4
FIRST_SHARES = (1, 1, 2)
LAST_SHARES = (2, 1, 1)
VMEM_LIMIT = 60 * 1024 * 1024


def wave_table(wavenumbers, lon_count):
    longitudes = jnp.arange(lon_count, dtype=jnp.int32)
    shifts = jnp.array([0, lon_count // 4], jnp.int32)[:, None]
    slots = wavenumbers.shape[-1]
    row_waves = jnp.broadcast_to(
        wavenumbers[..., None, :], wavenumbers.shape[:-1] + (2, slots)
    ).reshape(-1, 1)
    row_shifts = jnp.broadcast_to(shifts, wavenumbers.shape[:-1] + (2, slots)).reshape(-1, 1)
    phase = (row_waves * longitudes + row_shifts) % lon_count
    y = (phase - lon_count // 2).astype(jnp.float32) * (math.pi / lon_count)
    square = y * y
    series = jnp.full_like(square, 1.0 / math.factorial(13))
    for power in (11, 9, 7, 5, 3, 1):
        sign = 1.0 if power % 4 == 1 else -1.0
        series = series * square + sign / math.factorial(power)
    sine = y * series
    scaling = math.sqrt(2.0 / lon_count)
    return (sine * sine * (2.0 * scaling) - scaling).astype(jnp.bfloat16)


def part_ranges(items, shares):
    total, start, ranges = sum(shares), 0, []
    for share in shares:
        count = items * share // total
        ranges.append((start, count))
        start += count
    return ranges


def dft_kernel(table_ref, grid_ref, *out_refs):
    block, rows, lon_count = grid_ref.shape
    piece_rows = out_refs[0].shape[1]
    result = lax.dot_general(
        table_ref[...],
        grid_ref[...].reshape(block * rows, lon_count),
        (((1,), (1,)), ((), ())),
        preferred_element_type=jnp.float32,
    ).astype(jnp.bfloat16)
    for part, out_ref in enumerate(out_refs):
        for item in range(block):
            out_ref[item] = result[
                part * piece_rows : (part + 1) * piece_rows, item * rows : (item + 1) * rows
            ]


def forward_dft(table, grid_rows, parts, start, items):
    rows, lon_count = grid_rows.shape[1:]
    table_rows = table.shape[0]
    piece_rows = table_rows // parts
    block = 4
    return pl.pallas_call(
        dft_kernel,
        grid=(items // block,),
        in_specs=[
            pl.BlockSpec((table_rows, lon_count), lambda i: (0, 0)),
            pl.BlockSpec((block, rows, lon_count), lambda i: (i + start // block, 0, 0)),
        ],
        out_specs=[pl.BlockSpec((block, piece_rows, rows), lambda i: (i, 0, 0))] * parts,
        out_shape=[jax.ShapeDtypeStruct((items, piece_rows, rows), jnp.bfloat16)] * parts,
        compiler_params=pltpu.CompilerParams(vmem_limit_bytes=VMEM_LIMIT),
        cost_estimate=pl.CostEstimate(
            flops=2 * table_rows * items * rows * lon_count,
            bytes_accessed=2 * (items * rows * lon_count + items * rows * table_rows),
            transcendentals=0,
        ),
        name="forward_dft",
    )(table, grid_rows)


def inverse_kernel(piece_count, *refs):
    piece_refs = refs[:piece_count]
    table_ref, out_ref = refs[piece_count], refs[-1]
    block, rows, lon_count = out_ref.shape
    turned = []
    for item in range(block):
        column = jnp.concatenate([ref[item] for ref in piece_refs], axis=0)
        turned.append(column.T)
    left = jnp.concatenate(turned, axis=0)
    result = jnp.dot(left, table_ref[...], preferred_element_type=jnp.float32)
    out_ref[...] = result.astype(jnp.bfloat16).reshape(block, rows, lon_count)


def inverse_dft(pieces, offsets, table, start, items, all_items, held):
    _, piece_rows, rows = pieces[0].shape
    table_rows, lon_count = table.shape
    block = 4

    def piece_spec(offset):
        first = (start - offset) // block
        return pl.BlockSpec((block, piece_rows, rows), lambda i: (i + first, 0, 0))

    operands = [*pieces, table]
    in_specs = [piece_spec(offset) for offset in offsets]
    in_specs.append(pl.BlockSpec((table_rows, lon_count), lambda i: (0, 0)))
    aliases = {}
    if held is not None:
        aliases = {len(operands): 0}
        operands.append(held)
        in_specs.append(pl.BlockSpec(memory_space=pl.ANY))
    return pl.pallas_call(
        functools.partial(inverse_kernel, len(pieces)),
        grid=(items // block,),
        in_specs=in_specs,
        out_specs=pl.BlockSpec(
            (block, rows, lon_count), lambda i: (i + start // block, 0, 0)
        ),
        out_shape=jax.ShapeDtypeStruct((all_items, rows, lon_count), jnp.bfloat16),
        input_output_aliases=aliases,
        compiler_params=pltpu.CompilerParams(vmem_limit_bytes=VMEM_LIMIT),
        cost_estimate=pl.CostEstimate(
            flops=2 * table_rows * items * rows * lon_count,
            bytes_accessed=2 * (items * rows * lon_count + items * rows * table_rows),
            transcendentals=0,
        ),
        name="inverse_dft",
    )(*operands)


def legendre_kernel(in_count, out_ranges, wave_count, waves_ref, *refs):
    in_total = sum(in_count)
    flat_refs = refs[:in_total]
    piece_refs, at = [], 0
    for count in in_count:
        piece_refs.append(flat_refs[at : at + count])
        at += count
    legendre_ref, fold_ref, unfold_ref, weight_ref, params_ref = refs[in_total : in_total + 5]
    out_refs = refs[in_total + 5 : -2]
    fold_scratch, back_scratch = refs[-2:]
    items = sum(ref.shape[0] for ref in piece_refs[0])
    _, comps, slots, rows = piece_refs[0][0].shape
    merged = items * comps
    half = merged // 2
    width = legendre_ref.shape[3]
    norths = legendre_ref.shape[2]
    lanes = fold_scratch.shape[2]
    tiles = fold_scratch.shape[0]
    per_parity = tiles // 2

    gathered = jnp.concatenate(
        [
            jnp.concatenate(
                [ref[...].reshape(ref.shape[0] * comps * slots, rows) for ref in band], axis=0
            )
            for band in piece_refs
        ],
        axis=1,
    )
    for tile in range(tiles):
        columns = pl.ds(tile * lanes, lanes)
        fold_scratch[tile] = (
            jnp.dot(gathered, fold_ref[:, columns], preferred_element_type=jnp.float32)
            * weight_ref[:, columns]
        )

    first_slot = pl.program_id(0) * slots
    speed, depth, diffusion = params_ref[0], params_ref[1], params_ref[2]
    column_index = lax.broadcasted_iota(jnp.int32, (1, width), 1)

    def one_slot(slot, carry):
        wavenumber = waves_ref[first_slot + slot]
        picked = pl.ds(slot, merged, stride=slots)
        results = []
        for parity in range(2):
            source = jnp.concatenate(
                [
                    fold_scratch[parity * per_parity + tile, picked, :]
                    for tile in range(per_parity)
                ],
                axis=1,
            ).astype(jnp.bfloat16)
            table = legendre_ref[slot, parity]
            spectral = jnp.dot(source, table, preferred_element_type=jnp.float32)
            degree = wavenumber + 2 * column_index + parity
            eigen = (degree * (degree + 1)).astype(jnp.float32) * (
                1.0 / float(wave_count * (wave_count - 1))
            )
            divergence, geopotential = spectral[:half], spectral[half:]
            speed_eigen = speed * eigen
            new_div = (divergence + speed_eigen * geopotential) / (1.0 + speed_eigen * depth)
            new_geo = geopotential - depth * new_div
            damping = jnp.where(
                degree < wave_count, 1.0 / (1.0 + diffusion * (eigen * eigen)), 0.0
            )
            stepped = jnp.concatenate([new_div * damping, new_geo * damping], axis=0)
            results.append(
                lax.dot_general(
                    stepped.astype(jnp.bfloat16),
                    table,
                    (((1,), (1,)), ((), ())),
                    preferred_element_type=jnp.float32,
                )
            )
        north = results[0] + results[1]
        south = results[0] - results[1]
        for tile in range(per_parity):
            part = slice(tile * lanes, (tile + 1) * lanes)
            back_scratch[tile, picked, :] = north[:, part]
            back_scratch[per_parity + tile, picked, :] = south[:, part]
        return carry

    lax.fori_loop(0, slots, one_slot, 0, unroll=4)

    both = jnp.concatenate(
        [back_scratch[tile].astype(jnp.bfloat16) for tile in range(tiles)], axis=1
    )
    for part in range(len(piece_refs)):
        columns = pl.ds(part * rows, rows)
        result = jnp.dot(
            both, unfold_ref[:, columns], preferred_element_type=jnp.float32
        ).astype(jnp.bfloat16)
        for cut, (start, count) in enumerate(out_ranges):
            out_ref = out_refs[part * len(out_ranges) + cut]
            lines = slice(start * comps * slots, (start + count) * comps * slots)
            out_ref[...] = result[lines].reshape(count, comps, slots, rows)


def legendre_step(
    pieces, out_ranges, waves, legendre, chunk, fold, unfold, weights, params, wave_count
):
    items = sum(piece.shape[0] for piece in pieces[0])
    _, comps, slots, rows = pieces[0][0].shape
    _, parities, norths, width = legendre.shape
    block = 16 if slots % 16 == 0 else slots
    steps = slots // block
    merged = items * comps
    all_rows = fold.shape[0]
    lanes = min(128, norths)
    tiles = 2 * norths // lanes
    flat = [piece for band in pieces for piece in band]

    def piece_spec(count):
        return pl.BlockSpec((count, comps, block, rows), lambda i, w: (0, 0, i, 0))

    def whole(array):
        return pl.BlockSpec(array.shape, lambda i, w: (0,) * array.ndim)

    return pl.pallas_call(
        functools.partial(
            legendre_kernel, tuple(len(band) for band in pieces), out_ranges, wave_count
        ),
        grid_spec=pltpu.PrefetchScalarGridSpec(
            num_scalar_prefetch=1,
            grid=(steps,),
            in_specs=[piece_spec(piece.shape[0]) for piece in flat]
            + [
                pl.BlockSpec(
                    (block, parities, norths, width), lambda i, w: (chunk * steps + i, 0, 0, 0)
                ),
                whole(fold),
                whole(unfold),
                whole(weights),
                whole(params),
            ],
            out_specs=[piece_spec(count) for _, count in out_ranges] * len(pieces),
            scratch_shapes=[
                pltpu.VMEM((tiles, merged * block, lanes), jnp.float32),
                pltpu.VMEM((tiles, merged * block, lanes), jnp.float32),
            ],
        ),
        out_shape=[
            jax.ShapeDtypeStruct((count, comps, slots, rows), jnp.bfloat16)
            for _, count in out_ranges
        ]
        * len(pieces),
        compiler_params=pltpu.CompilerParams(vmem_limit_bytes=VMEM_LIMIT),
        cost_estimate=pl.CostEstimate(
            flops=2 * slots * merged * (4 * norths * width + 2 * all_rows * all_rows),
            bytes_accessed=2
            * (slots * parities * norths * width + 2 * slots * merged * all_rows),
            transcendentals=0,
        ),
        name="legendre_step",
    )(waves, *flat, legendre, fold, unfold, weights, params)


def per_device(
    size,
    grid_fields,
    band_latitude,
    wave_of_slot,
    legendre,
    quad_weight,
    wave_speed,
    layer_depth,
    diffusion,
):
    field_count, lev_dev, lat_dev, lon_count = grid_fields.shape
    wave_count = wave_of_slot.shape[0]
    north_count = quad_weight.shape[0]
    half_band = lat_dev // 2
    slot_count = legendre.shape[0]
    width = legendre.shape[3]
    chunk_slots = slot_count // CHUNKS
    items = field_count * lev_dev
    me = lax.axis_index("wave")
    partners = jnp.bitwise_xor(me, jnp.arange(size, dtype=jnp.int32))

    level_start = lax.axis_index("lev") * lev_dev
    params = jnp.stack(
        [
            jnp.broadcast_to(
                jnp.repeat(lax.dynamic_slice_in_dim(values, level_start, lev_dev, 0), 2)[:, None],
                (2 * lev_dev, width),
            )
            for values in (wave_speed, layer_depth, diffusion)
        ]
    )

    waves = wave_of_slot.reshape(size, CHUNKS, chunk_slots)[partners]
    my_waves = waves[0]

    row_lat = band_latitude.reshape(size, lat_dev)[partners].reshape(size * lat_dev)
    lats = jnp.arange(north_count, dtype=jnp.int32)
    is_north = (row_lat[:, None] == lats[None, :]).astype(jnp.bfloat16)
    is_south = (row_lat[:, None] == 2 * north_count - 1 - lats[None, :]).astype(jnp.bfloat16)
    fold = jnp.concatenate([is_north + is_south, is_north - is_south], axis=1)
    unfold = jnp.concatenate([is_north, is_south], axis=1).T
    weights = jnp.concatenate([quad_weight, quad_weight])[None, :]

    def send(piece, offset):
        if offset == 0:
            return piece
        return lax.ppermute(piece, "wave", [(index, index ^ offset) for index in range(size)])

    grid_rows = grid_fields.reshape(items, lat_dev, lon_count)
    aligned = lat_dev % 128 == 0
    whole = [(0, items)]
    arrived = []
    tables = []
    chunk_waves = waves
    for chunk in range(CHUNKS):
        tables.append(wave_table(chunk_waves[:, chunk], lon_count))
        bands = [[] for _ in range(size)]
        for start, count in part_ranges(items, FIRST_SHARES) if chunk == 0 else whole:
            pieces = forward_dft(tables[chunk], grid_rows, size, start, count)
            chunk_waves, _ = lax.optimization_barrier((waves, pieces[-1]))
            for offset, piece in enumerate(pieces):
                bands[offset].append(
                    send(piece, offset).reshape(count, 2, chunk_slots, lat_dev)
                )
        arrived.append(bands)
    returned = []
    for chunk in range(CHUNKS):
        bands = arrived[chunk]
        ranges = part_ranges(items, LAST_SHARES) if chunk == CHUNKS - 1 else whole
        if not aligned:
            bands = [[jnp.concatenate([jnp.concatenate(band, axis=0) for band in bands], axis=3)]]
        backs = legendre_step(
            bands, ranges, my_waves[chunk], legendre, chunk, fold, unfold, weights, params,
            wave_count,
        )
        if not aligned:
            split = [jnp.split(back, size, axis=3) for back in backs]
            backs = [split[cut][offset] for offset in range(size) for cut in range(len(ranges))]
        sent = {}
        for cut, (start, count) in enumerate(ranges):
            for offset in range(size):
                back = backs[offset * len(ranges) + cut]
                sent[cut, offset] = send(back.reshape(count, 2 * chunk_slots, lat_dev), offset)
        returned.append((ranges, sent))
    table = jnp.concatenate(tables, axis=0)
    grid_out = None
    for last_cut, (start, count) in enumerate(part_ranges(items, LAST_SHARES)):
        pieces, offsets = [], []
        for ranges, sent in returned:
            cut = last_cut if len(ranges) > 1 else 0
            pieces += [sent[cut, offset] for offset in range(size)]
            offsets += [ranges[cut][0]] * size
        grid_out = inverse_dft(pieces, offsets, table, start, count, items, grid_out)
    return grid_out.reshape(field_count, lev_dev, lat_dev, lon_count)


def solution(mesh):
    in_specs = (
        P("member", "lev", "wave", None),
        P(),
        P(),
        P("wave", None, None, None),
        P(),
        P("member"),
        P("member"),
        P("member"),
    )
    out_specs = P("member", "lev", "wave", None)
    return jax.shard_map(
        functools.partial(per_device, mesh.shape["wave"]),
        mesh=mesh,
        in_specs=in_specs,
        out_specs=out_specs,
        check_vma=False,
    )
```

```python
import functools
import math

import jax
import jax.numpy as jnp
from jax import lax
from jax.experimental import pallas as pl
from jax.experimental.pallas import tpu as pltpu
from jax.sharding import PartitionSpec as P

CHUNKS = 4
SEND_SHARES = {0: (1, 1, 2), 1: (1, 1)}
LAST_SHARES = (4, 2, 1, 1)
CUT_FROM = CHUNKS - 2
VMEM_LIMIT = 60 * 1024 * 1024


def wave_table(wavenumbers, lon_count):
    longitudes = jnp.arange(lon_count, dtype=jnp.int32)
    shifts = jnp.array([0, lon_count // 4], jnp.int32)[:, None]
    slots = wavenumbers.shape[-1]
    row_waves = jnp.broadcast_to(
        wavenumbers[..., None, :], wavenumbers.shape[:-1] + (2, slots)
    ).reshape(-1, 1)
    row_shifts = jnp.broadcast_to(shifts, wavenumbers.shape[:-1] + (2, slots)).reshape(-1, 1)
    phase = (row_waves * longitudes + row_shifts) % lon_count
    y = (phase - lon_count // 2).astype(jnp.float32) * (math.pi / lon_count)
    square = y * y
    series = jnp.full_like(square, 1.0 / math.factorial(13))
    for power in (11, 9, 7, 5, 3, 1):
        sign = 1.0 if power % 4 == 1 else -1.0
        series = series * square + sign / math.factorial(power)
    sine = y * series
    scaling = math.sqrt(2.0 / lon_count)
    return (sine * sine * (2.0 * scaling) - scaling).astype(jnp.bfloat16)


def part_ranges(items, shares):
    total, start, ranges = sum(shares), 0, []
    for share in shares:
        count = items * share // total
        ranges.append((start, count))
        start += count
    return ranges


def dft_kernel(table_ref, grid_ref, *out_refs):
    block, rows, lon_count = grid_ref.shape
    piece_rows = out_refs[0].shape[1]
    result = lax.dot_general(
        table_ref[...],
        grid_ref[...].reshape(block * rows, lon_count),
        (((1,), (1,)), ((), ())),
        preferred_element_type=jnp.float32,
    ).astype(jnp.bfloat16)
    for part, out_ref in enumerate(out_refs):
        for item in range(block):
            out_ref[item] = result[
                part * piece_rows : (part + 1) * piece_rows, item * rows : (item + 1) * rows
            ]


def forward_dft(table, grid_rows, parts, start, items):
    rows, lon_count = grid_rows.shape[1:]
    table_rows = table.shape[0]
    piece_rows = table_rows // parts
    block = 4
    return pl.pallas_call(
        dft_kernel,
        grid=(items // block,),
        in_specs=[
            pl.BlockSpec((table_rows, lon_count), lambda i: (0, 0)),
            pl.BlockSpec((block, rows, lon_count), lambda i: (i + start // block, 0, 0)),
        ],
        out_specs=[pl.BlockSpec((block, piece_rows, rows), lambda i: (i, 0, 0))] * parts,
        out_shape=[jax.ShapeDtypeStruct((items, piece_rows, rows), jnp.bfloat16)] * parts,
        compiler_params=pltpu.CompilerParams(vmem_limit_bytes=VMEM_LIMIT),
        cost_estimate=pl.CostEstimate(
            flops=2 * table_rows * items * rows * lon_count,
            bytes_accessed=2 * (items * rows * lon_count + items * rows * table_rows),
            transcendentals=0,
        ),
        name="forward_dft",
    )(table, grid_rows)


def inverse_kernel(piece_count, *refs):
    piece_refs = refs[:piece_count]
    table_ref, out_ref = refs[piece_count], refs[-1]
    block, rows, lon_count = out_ref.shape
    turned = []
    for item in range(block):
        column = jnp.concatenate([ref[item] for ref in piece_refs], axis=0)
        turned.append(column.T)
    left = jnp.concatenate(turned, axis=0)
    result = jnp.dot(left, table_ref[...], preferred_element_type=jnp.float32)
    out_ref[...] = result.astype(jnp.bfloat16).reshape(block, rows, lon_count)


def inverse_dft(pieces, offsets, table, start, items, all_items, held):
    _, piece_rows, rows = pieces[0].shape
    table_rows, lon_count = table.shape
    block = 4

    def piece_spec(offset):
        first = (start - offset) // block
        return pl.BlockSpec((block, piece_rows, rows), lambda i: (i + first, 0, 0))

    operands = [*pieces, table]
    in_specs = [piece_spec(offset) for offset in offsets]
    in_specs.append(pl.BlockSpec((table_rows, lon_count), lambda i: (0, 0)))
    aliases = {}
    if held is not None:
        aliases = {len(operands): 0}
        operands.append(held)
        in_specs.append(pl.BlockSpec(memory_space=pl.ANY))
    return pl.pallas_call(
        functools.partial(inverse_kernel, len(pieces)),
        grid=(items // block,),
        in_specs=in_specs,
        out_specs=pl.BlockSpec(
            (block, rows, lon_count), lambda i: (i + start // block, 0, 0)
        ),
        out_shape=jax.ShapeDtypeStruct((all_items, rows, lon_count), jnp.bfloat16),
        input_output_aliases=aliases,
        compiler_params=pltpu.CompilerParams(vmem_limit_bytes=VMEM_LIMIT),
        cost_estimate=pl.CostEstimate(
            flops=2 * table_rows * items * rows * lon_count,
            bytes_accessed=2 * (items * rows * lon_count + items * rows * table_rows),
            transcendentals=0,
        ),
        name="inverse_dft",
    )(*operands)


def legendre_kernel(in_count, out_ranges, wave_count, waves_ref, *refs):
    in_total = sum(in_count)
    flat_refs = refs[:in_total]
    piece_refs, at = [], 0
    for count in in_count:
        piece_refs.append(flat_refs[at : at + count])
        at += count
    legendre_ref, fold_ref, unfold_ref, weight_ref, params_ref = refs[in_total : in_total + 5]
    out_refs = refs[in_total + 5 : -2]
    fold_scratch, back_scratch = refs[-2:]
    items = sum(ref.shape[0] for ref in piece_refs[0])
    _, comps, slots, rows = piece_refs[0][0].shape
    merged = items * comps
    half = merged // 2
    width = legendre_ref.shape[3]
    norths = legendre_ref.shape[2]
    lanes = fold_scratch.shape[2]
    tiles = fold_scratch.shape[0]
    per_parity = tiles // 2

    gathered = jnp.concatenate(
        [
            jnp.concatenate(
                [ref[...].reshape(ref.shape[0] * comps * slots, rows) for ref in band], axis=0
            )
            for band in piece_refs
        ],
        axis=1,
    )
    for tile in range(tiles):
        columns = pl.ds(tile * lanes, lanes)
        fold_scratch[tile] = (
            jnp.dot(gathered, fold_ref[:, columns], preferred_element_type=jnp.float32)
            * weight_ref[:, columns]
        )

    first_slot = pl.program_id(0) * slots
    speed, depth, diffusion = params_ref[0], params_ref[1], params_ref[2]
    column_index = lax.broadcasted_iota(jnp.int32, (1, width), 1)

    def one_slot(slot, carry):
        wavenumber = waves_ref[first_slot + slot]
        picked = pl.ds(slot, merged, stride=slots)
        results = []
        for parity in range(2):
            source = jnp.concatenate(
                [
                    fold_scratch[parity * per_parity + tile, picked, :]
                    for tile in range(per_parity)
                ],
                axis=1,
            ).astype(jnp.bfloat16)
            table = legendre_ref[slot, parity]
            spectral = jnp.dot(source, table, preferred_element_type=jnp.float32)
            degree = wavenumber + 2 * column_index + parity
            eigen = (degree * (degree + 1)).astype(jnp.float32) * (
                1.0 / float(wave_count * (wave_count - 1))
            )
            divergence, geopotential = spectral[:half], spectral[half:]
            speed_eigen = speed * eigen
            new_div = (divergence + speed_eigen * geopotential) / (1.0 + speed_eigen * depth)
            new_geo = geopotential - depth * new_div
            damping = jnp.where(
                degree < wave_count, 1.0 / (1.0 + diffusion * (eigen * eigen)), 0.0
            )
            stepped = jnp.concatenate([new_div * damping, new_geo * damping], axis=0)
            results.append(
                lax.dot_general(
                    stepped.astype(jnp.bfloat16),
                    table,
                    (((1,), (1,)), ((), ())),
                    preferred_element_type=jnp.float32,
                )
            )
        north = results[0] + results[1]
        south = results[0] - results[1]
        for tile in range(per_parity):
            part = slice(tile * lanes, (tile + 1) * lanes)
            back_scratch[tile, picked, :] = north[:, part]
            back_scratch[per_parity + tile, picked, :] = south[:, part]
        return carry

    lax.fori_loop(0, slots, one_slot, 0, unroll=4)

    both = jnp.concatenate(
        [back_scratch[tile].astype(jnp.bfloat16) for tile in range(tiles)], axis=1
    )
    for part in range(len(piece_refs)):
        columns = pl.ds(part * rows, rows)
        result = jnp.dot(
            both, unfold_ref[:, columns], preferred_element_type=jnp.float32
        ).astype(jnp.bfloat16)
        for cut, (start, count) in enumerate(out_ranges):
            out_ref = out_refs[part * len(out_ranges) + cut]
            lines = slice(start * comps * slots, (start + count) * comps * slots)
            out_ref[...] = result[lines].reshape(count, comps, slots, rows)


def legendre_step(
    pieces, out_ranges, waves, legendre, chunk, fold, unfold, weights, params, wave_count
):
    items = sum(piece.shape[0] for piece in pieces[0])
    _, comps, slots, rows = pieces[0][0].shape
    _, parities, norths, width = legendre.shape
    block = 16 if slots % 16 == 0 else slots
    steps = slots // block
    merged = items * comps
    all_rows = fold.shape[0]
    lanes = min(128, norths)
    tiles = 2 * norths // lanes
    flat = [piece for band in pieces for piece in band]

    def piece_spec(count):
        return pl.BlockSpec((count, comps, block, rows), lambda i, w: (0, 0, i, 0))

    def whole(array):
        return pl.BlockSpec(array.shape, lambda i, w: (0,) * array.ndim)

    return pl.pallas_call(
        functools.partial(
            legendre_kernel, tuple(len(band) for band in pieces), out_ranges, wave_count
        ),
        grid_spec=pltpu.PrefetchScalarGridSpec(
            num_scalar_prefetch=1,
            grid=(steps,),
            in_specs=[piece_spec(piece.shape[0]) for piece in flat]
            + [
                pl.BlockSpec(
                    (block, parities, norths, width), lambda i, w: (chunk * steps + i, 0, 0, 0)
                ),
                whole(fold),
                whole(unfold),
                whole(weights),
                whole(params),
            ],
            out_specs=[piece_spec(count) for _, count in out_ranges] * len(pieces),
            scratch_shapes=[
                pltpu.VMEM((tiles, merged * block, lanes), jnp.float32),
                pltpu.VMEM((tiles, merged * block, lanes), jnp.float32),
            ],
        ),
        out_shape=[
            jax.ShapeDtypeStruct((count, comps, slots, rows), jnp.bfloat16)
            for _, count in out_ranges
        ]
        * len(pieces),
        compiler_params=pltpu.CompilerParams(vmem_limit_bytes=VMEM_LIMIT),
        cost_estimate=pl.CostEstimate(
            flops=2 * slots * merged * (4 * norths * width + 2 * all_rows * all_rows),
            bytes_accessed=2
            * (slots * parities * norths * width + 2 * slots * merged * all_rows),
            transcendentals=0,
        ),
        name="legendre_step",
    )(waves, *flat, legendre, fold, unfold, weights, params)


def per_device(
    size,
    grid_fields,
    band_latitude,
    wave_of_slot,
    legendre,
    quad_weight,
    wave_speed,
    layer_depth,
    diffusion,
):
    field_count, lev_dev, lat_dev, lon_count = grid_fields.shape
    wave_count = wave_of_slot.shape[0]
    north_count = quad_weight.shape[0]
    half_band = lat_dev // 2
    slot_count = legendre.shape[0]
    width = legendre.shape[3]
    chunk_slots = slot_count // CHUNKS
    items = field_count * lev_dev
    me = lax.axis_index("wave")
    partners = jnp.bitwise_xor(me, jnp.arange(size, dtype=jnp.int32))

    level_start = lax.axis_index("lev") * lev_dev
    params = jnp.stack(
        [
            jnp.broadcast_to(
                jnp.repeat(lax.dynamic_slice_in_dim(values, level_start, lev_dev, 0), 2)[:, None],
                (2 * lev_dev, width),
            )
            for values in (wave_speed, layer_depth, diffusion)
        ]
    )

    waves = wave_of_slot.reshape(size, CHUNKS, chunk_slots)[partners]
    my_waves = waves[0]

    row_lat = band_latitude.reshape(size, lat_dev)[partners].reshape(size * lat_dev)
    lats = jnp.arange(north_count, dtype=jnp.int32)
    is_north = (row_lat[:, None] == lats[None, :]).astype(jnp.bfloat16)
    is_south = (row_lat[:, None] == 2 * north_count - 1 - lats[None, :]).astype(jnp.bfloat16)
    fold = jnp.concatenate([is_north + is_south, is_north - is_south], axis=1)
    unfold = jnp.concatenate([is_north, is_south], axis=1).T
    weights = jnp.concatenate([quad_weight, quad_weight])[None, :]

    def send(piece, offset):
        if offset == 0:
            return piece
        return lax.ppermute(piece, "wave", [(index, index ^ offset) for index in range(size)])

    grid_rows = grid_fields.reshape(items, lat_dev, lon_count)
    aligned = lat_dev % 128 == 0
    whole = [(0, items)]
    arrived = []
    tables = []
    chunk_waves = waves
    for chunk in range(CHUNKS):
        tables.append(wave_table(chunk_waves[:, chunk], lon_count))
        bands = [[] for _ in range(size)]
        for start, count in part_ranges(items, SEND_SHARES.get(chunk, (1,))):
            pieces = forward_dft(tables[chunk], grid_rows, size, start, count)
            chunk_waves, _ = lax.optimization_barrier((waves, pieces[-1]))
            sends = {offset: send(pieces[offset], offset) for offset in reversed(range(size))}
            for offset in range(size):
                bands[offset].append(
                    sends[offset].reshape(count, 2, chunk_slots, lat_dev)
                )
        arrived.append(bands)
    returned = []
    for chunk in range(CHUNKS):
        bands = arrived[chunk]
        ranges = part_ranges(items, LAST_SHARES) if chunk >= CUT_FROM else whole
        if not aligned:
            bands = [[jnp.concatenate([jnp.concatenate(band, axis=0) for band in bands], axis=3)]]
        backs = legendre_step(
            bands, ranges, my_waves[chunk], legendre, chunk, fold, unfold, weights, params,
            wave_count,
        )
        if not aligned:
            split = [jnp.split(back, size, axis=3) for back in backs]
            backs = [split[cut][offset] for offset in range(size) for cut in range(len(ranges))]
        pieces = {
            (cut, offset): backs[offset * len(ranges) + cut].reshape(
                ranges[cut][1], 2 * chunk_slots, lat_dev
            )
            for cut in range(len(ranges))
            for offset in range(size)
        }
        returned.append((ranges, pieces, {}))
    for ranges, pieces, sent in returned:
        for offset in reversed(range(size)):
            sent[0, offset] = send(pieces[0, offset], offset)
    last = returned[-1][1][0, size - 1]
    for cut in range(1, len(LAST_SHARES)):
        for ranges, pieces, sent in returned[CUT_FROM:]:
            for offset in reversed(range(size)):
                piece, last = lax.optimization_barrier((pieces[cut, offset], last))
                sent[cut, offset] = send(piece, offset)
    table = jnp.concatenate(tables, axis=0)
    grid_out = None
    for last_cut, (start, count) in enumerate(part_ranges(items, LAST_SHARES)):
        pieces, offsets = [], []
        for ranges, _, sent in returned:
            cut = last_cut if len(ranges) > 1 else 0
            pieces += [sent[cut, offset] for offset in range(size)]
            offsets += [ranges[cut][0]] * size
        grid_out = inverse_dft(pieces, offsets, table, start, count, items, grid_out)
    return grid_out.reshape(field_count, lev_dev, lat_dev, lon_count)


def solution(mesh):
    in_specs = (
        P("member", "lev", "wave", None),
        P(),
        P(),
        P("wave", None, None, None),
        P(),
        P("member"),
        P("member"),
        P("member"),
    )
    out_specs = P("member", "lev", "wave", None)
    return jax.shard_map(
        functools.partial(per_device, mesh.shape["wave"]),
        mesh=mesh,
        in_specs=in_specs,
        out_specs=out_specs,
        check_vma=False,
    )
```
